32 devices in a mesh: grp: 1, sp: 32 (over z, y, x, core), ch: 1.
Axes of the slice: x: 2, y: 2, z: 4, core: 2. Of those that a mesh axis runs over, the one named last changes fastest.
Arguments:
- latents: bfloat16 [131072, 1024], P(('grp', 'sp')), may hold values from -6 to 6
- spectrum: bfloat16 [16, 64, 128, 1024], P(None, None, 'sp', 'ch'), may hold values from -4 to 4
- w_value: bfloat16 [1024, 1024], P('sp', 'ch'), may hold values from -0.1875 to 0.1875
- w_gate: bfloat16 [1024, 1024], P('sp', 'ch'), may hold values from -0.1875 to 0.1875
- w_out: bfloat16 [1024, 1024], P('sp'), may hold values from -0.1875 to 0.1875
- embed_table: bfloat16 [1024, 32768], P(('sp', 'ch')), may hold values from -12 to 12
- prompt_ids: int32 [256], P('grp'), may hold values from 0 to 32767
- noise_step: int32 [1], P('grp'), may hold values from 0 to 999
Outputs:
- denoised: bfloat16 [131072, 1024], P(('grp', 'sp', 'ch'))
The draws below stay inside these ranges and needn't reach their ends.
All inputs are finite; a program needn't handle non-finite values.
Results may differ from the reference program's by a relative error of at most 0.013.
Values may be sent and summed in bfloat16 or wider, within the bound.
A program may use at most 128 MiB of HBM per device.

```python
import math
import jax
import jax.numpy as jnp
import numpy as np
from jax import lax

TT = 16
HH = 64
WW = 128
C = 1024
VOCAB = 32768
PROMPT = 256
CELLS = 131072


def plant(drawn, own_key, low, high):
    longest = drawn.shape.index(max(drawn.shape))
    spots = []
    for shift in (0, 1):
        where = [jax.random.randint(jax.random.fold_in(own_key, axis), (), 0, length) for axis, length in enumerate(drawn.shape)]
        where[longest] = (where[longest] + shift) % drawn.shape[longest]
        spots.append(tuple(where))
    return drawn.at[spots[0]].set(low).at[spots[1]].set(high)


def shard_levels(key, dims, cuts, least, top_value):
    loudness, own = 1.0, jax.random.fold_in(key, 6)
    for axis_at, shards_of in cuts:
        draws = jnp.exp(jax.random.uniform(jax.random.fold_in(own, axis_at), (shards_of,), jnp.float32, least / len(cuts), top_value / len(cuts)))
        loudness = loudness * jnp.repeat(draws, dims[axis_at] // shards_of).reshape([-1 if axis == axis_at else 1 for axis in range(len(dims))])
    return loudness


def rank_table(amount, slope):
    weights = [(1 << 20) // math.isqrt(grade ** slope) + 1 for grade in range(1, amount + 1)]
    width = 1 + sum(weights) // (1 << 30)
    return np.cumsum(np.array([max(1, weight // width) for weight in weights]))


def ranked(key, dims, count, lean):
    table = rank_table(count, lean)
    lot = jax.random.randint(jax.random.fold_in(key, 1), dims, 0, int(table[count - 1]))
    rank = jnp.searchsorted(jnp.asarray(table, jnp.int32), lot, side="right")
    return jax.random.permutation(jax.random.fold_in(key, 2), count)[rank].astype(jnp.int32)


def bell_draw(own_key, dims, scale, limit, cuts=(), held_as=jnp.bfloat16):
    values = scale * jax.random.normal(own_key, dims, jnp.float32)
    if cuts:
        values = values * shard_levels(own_key, dims, cuts, -0.22, 0.18)
    return jnp.clip(values, -limit, limit).astype(held_as)


def setup_inputs(seed: int = 0, part: int = 0) -> dict:
    key_list = jax.random.split(jax.random.key(seed), 9)
    part_keys = jax.random.split(jax.random.fold_in(key_list[8], part), 9)
    latents = bell_draw(part_keys[0], (CELLS, C), 1.0, 6.0, ((0, 32),))
    spectrum = bell_draw(key_list[1], (TT, HH, WW, C), 1.0, 4.0, ((2, 32),))
    w_value = bell_draw(key_list[2], (C, C), C ** -0.5, 0.1875, ((0, 32),))
    w_gate = bell_draw(key_list[3], (C, C), C ** -0.5, 0.1875, ((0, 32),))
    w_out = bell_draw(key_list[4], (C, C), C ** -0.5, 0.1875, ((0, 32),))
    embed_table = bell_draw(key_list[5], (C, VOCAB), 3.0, 12.0, ((0, 32),))
    prompt_ids = plant(ranked(part_keys[6], (PROMPT,), VOCAB, 2), jax.random.fold_in(part_keys[6], 3), 0, VOCAB - 1).astype(jnp.int32)
    noise_step = jax.random.randint(part_keys[7], (1,), 0, 1000).astype(jnp.int32)
    return {"latents": latents, "spectrum": spectrum, "w_value": w_value, "w_gate": w_gate, "w_out": w_out, "embed_table": embed_table, "prompt_ids": prompt_ids, "noise_step": noise_step}


def cas_table(length):
    position = jnp.arange(length, dtype=jnp.int32)
    product = position[:, None] * position[None, :] % length
    phase_angle = product.astype(jnp.float32) * (2.0 * math.pi / length)
    return ((jnp.cos(phase_angle) + jnp.sin(phase_angle)) / math.sqrt(length)).astype(jnp.bfloat16)

def step_embedding(noise_step, channel, channels):
    half_count = channels // 2
    lower_half = channel < half_count
    position = jnp.where(lower_half, channel, channel - half_count).astype(jnp.float32)
    frequency = jnp.exp(-math.log(10000.0) * position / half_count)
    phase_angle = noise_step[0].astype(jnp.float32) * frequency
    return jnp.where(lower_half, jnp.sin(phase_angle), jnp.cos(phase_angle))

def apply_table(form, table, operand):
    return jnp.einsum(form, table.astype(jnp.float32), operand.astype(jnp.float32), precision=lax.Precision.HIGHEST)

def reference(latents, spectrum, w_value, w_gate, w_out, embed_table, prompt_ids, noise_step):
    channel = jnp.arange(C, dtype=jnp.int32)
    pooled = lax.optimization_barrier(jnp.mean(jnp.take(embed_table, prompt_ids, axis=1).astype(jnp.float32), axis=1))
    modulation = 1.0 + pooled + step_embedding(noise_step, channel, C)
    value_rows = jnp.dot(latents, w_value, preferred_element_type=jnp.float32).astype(jnp.bfloat16)
    gate_rows = jnp.dot(latents, w_gate, preferred_element_type=jnp.float32)
    cas_width = cas_table(WW)
    cas_height = cas_table(HH)
    cas_time = cas_table(TT)
    latent_grid = value_rows.reshape(TT, HH, WW, C)
    width_spec = apply_table('kw,thwc->thkc', cas_width, latent_grid).astype(jnp.bfloat16)
    height_spec = apply_table('ah,thkc->takc', cas_height, width_spec).astype(jnp.bfloat16)
    full_spec = apply_table('st,takc->sakc', cas_time, height_spec).astype(jnp.bfloat16)
    filtered = (full_spec.astype(jnp.float32) * spectrum.astype(jnp.float32)).astype(jnp.bfloat16)
    time_back = apply_table('ts,sakc->takc', cas_time, filtered).astype(jnp.bfloat16)
    height_back = apply_table('ha,takc->thkc', cas_height, time_back).astype(jnp.bfloat16)
    mix_rows = apply_table('wk,thkc->thwc', cas_width, height_back).reshape(TT * HH * WW, C)
    mixed_rows = (mix_rows * jax.nn.silu(gate_rows) * modulation[None, :]).astype(jnp.bfloat16)
    projected = jnp.dot(mixed_rows, w_out, preferred_element_type=jnp.float32)
    return (latents.astype(jnp.float32) + projected).astype(jnp.bfloat16)
```

```python
import math

import jax
import jax.numpy as jnp
import numpy as np
from jax import lax
from jax.experimental import pallas as pl
from jax.experimental.pallas import tpu as pltpu
from jax.sharding import PartitionSpec as P

TT = 16
HH = 64
WW = 128
C = 1024

TILE = 16


def cas_table(length):
    position = jnp.arange(length, dtype=jnp.int32)
    product = position[:, None] * position[None, :] % length
    phase_angle = product.astype(jnp.float32) * (2.0 * math.pi / length)
    return ((jnp.cos(phase_angle) + jnp.sin(phase_angle)) / math.sqrt(length)).astype(jnp.bfloat16)


def step_embedding(noise_step, channel, channels):
    half_count = channels // 2
    lower_half = channel < half_count
    position = jnp.where(lower_half, channel, channel - half_count).astype(jnp.float32)
    frequency = jnp.exp(-math.log(10000.0) * position / half_count)
    phase_angle = noise_step[0].astype(jnp.float32) * frequency
    return jnp.where(lower_half, jnp.sin(phase_angle), jnp.cos(phase_angle))


def widened(table, copies):
    length = table.shape[0]
    inner = jnp.eye(copies, dtype=table.dtype)
    both = table[:, None, :, None] * inner[None, :, None, :]
    return both.reshape(length * copies, length * copies)


def dot(left, right):
    return jnp.dot(left, right, preferred_element_type=jnp.float32)


def width_kernel(table_ref, latents_ref, out_ref):
    owners, rows, channels = out_ref.shape
    moved = dot(table_ref[...], latents_ref[...])
    out_ref[...] = moved.reshape(owners, rows, channels).astype(out_ref.dtype)


def width_forward(table, latents, owners, lines, band, group):
    channels = latents.shape[1]
    rows = group * WW
    cells = lines * WW
    return pl.pallas_call(
        width_kernel,
        grid=(lines // group,),
        in_specs=[
            pl.BlockSpec(table.shape, lambda g: (0, 0)),
            pl.BlockSpec((rows, channels), lambda g: (g, 0)),
        ],
        out_specs=pl.BlockSpec((owners, group * band, channels), lambda g: (0, g, 0)),
        out_shape=jax.ShapeDtypeStruct((owners, lines * band, channels), jnp.bfloat16),
        compiler_params=pltpu.CompilerParams(vmem_limit_bytes=48 * 2**20),
        cost_estimate=pl.CostEstimate(
            flops=2 * cells * table.shape[0] * channels,
            bytes_accessed=4 * cells * channels,
            transcendentals=0,
        ),
        name="width_forward",
    )(table, latents)


def plane_kernel(band, height_ref, time_ref, planes_ref, weight_ref, spectrum_ref, out_ref, spec):
    per_frame = HH * band
    width = out_ref.shape[1]
    pieces = per_frame // TILE
    weight = weight_ref[...].reshape(planes_ref.shape[1], width)

    def forward(t, carry):
        rows = pl.ds(pl.multiple_of(t * per_frame, per_frame), per_frame)
        value = dot(planes_ref[rows, :], weight).astype(jnp.bfloat16)
        spec[t] = dot(height_ref[...], value).astype(jnp.bfloat16)
        return carry

    lax.fori_loop(0, TT, forward, 0, unroll=4)

    def across(p, carry):
        rows = pl.ds(pl.multiple_of(p * TILE, TILE), TILE)
        block = spec[:, rows, :].reshape(TT * TILE, width)
        full = dot(time_ref[...], block)
        gain = spectrum_ref[:, rows, :].reshape(TT * TILE, width).astype(jnp.float32)
        filtered = (full * gain).astype(jnp.bfloat16)
        back = dot(time_ref[...], filtered).astype(jnp.bfloat16)
        spec[:, rows, :] = back.reshape(TT, TILE, width)
        return carry

    lax.fori_loop(0, pieces, across, 0, unroll=4)

    def backward(t, carry):
        rows = pl.ds(pl.multiple_of(t * per_frame, per_frame), per_frame)
        out_ref[rows, :] = dot(height_ref[...], spec[t]).astype(jnp.bfloat16)
        return carry

    lax.fori_loop(0, TT, backward, 0, unroll=4)


def plane_filter(height, time, planes, weight, spectrum, band):
    cells, channels = planes.shape
    shards, depth, chan_part = weight.shape
    width = min(256, chan_part)
    per_frame = HH * band
    return pl.pallas_call(
        lambda *refs: plane_kernel(band, *refs),
        grid=(chan_part // width,),
        in_specs=[
            pl.BlockSpec(height.shape, lambda g: (0, 0)),
            pl.BlockSpec(time.shape, lambda g: (0, 0)),
            pl.BlockSpec((cells, channels), lambda g: (0, 0)),
            pl.BlockSpec((shards, depth, width), lambda g: (0, 0, g)),
            pl.BlockSpec((TT, per_frame, width), lambda g: (0, 0, g)),
        ],
        out_specs=pl.BlockSpec((cells, width), lambda g: (0, g)),
        out_shape=jax.ShapeDtypeStruct((cells, chan_part), jnp.bfloat16),
        scratch_shapes=[pltpu.VMEM((TT, per_frame, width), jnp.bfloat16)],
        cost_estimate=pl.CostEstimate(
            flops=2 * cells * chan_part * (channels + 1024),
            bytes_accessed=2 * cells * (channels + 2 * chan_part),
            transcendentals=0,
        ),
        compiler_params=pltpu.CompilerParams(vmem_limit_bytes=56 * 2**20),
        name="plane_filter",
    )(height, time, planes, weight, spectrum)


def gate_kernel(latents_ref, gate_ref, scale_ref, out_ref):
    gate = dot(latents_ref[...], gate_ref[...].reshape(latents_ref.shape[1], out_ref.shape[1]))
    gate = gate / (1.0 + jnp.exp(-gate))
    out_ref[...] = (gate * scale_ref[...]).astype(out_ref.dtype)


def gate_rows(latents, gate_w, scale):
    cells, channels = latents.shape
    chan_part = gate_w.shape[2]
    rows = min(512, cells)
    return pl.pallas_call(
        gate_kernel,
        grid=(cells // rows,),
        in_specs=[
            pl.BlockSpec((rows, channels), lambda g: (g, 0)),
            pl.BlockSpec(gate_w.shape, lambda g: (0, 0, 0)),
            pl.BlockSpec((1, chan_part), lambda g: (0, 0)),
        ],
        out_specs=pl.BlockSpec((rows, chan_part), lambda g: (g, 0)),
        out_shape=jax.ShapeDtypeStruct((cells, chan_part), jnp.bfloat16),
        compiler_params=pltpu.CompilerParams(vmem_limit_bytes=48 * 2**20),
        cost_estimate=pl.CostEstimate(
            flops=2 * cells * channels * chan_part,
            bytes_accessed=2 * cells * (channels + chan_part),
            transcendentals=cells * chan_part,
        ),
        name="gate_rows",
    )(latents, gate_w, scale)


def mix_kernel(parts, residual, *refs):
    tables, backs = refs[:parts], refs[parts : 2 * parts]
    latents_ref, gate_ref, out_w_ref, out_ref = refs[2 * parts :]
    owners, rows, chan_part = backs[0].shape
    mix = dot(tables[0][...], backs[0][...].reshape(owners * rows, chan_part))
    for table_ref, back_ref in zip(tables[1:], backs[1:]):
        mix += dot(table_ref[...], back_ref[...].reshape(owners * rows, chan_part))
    mixed = (mix * gate_ref[...].astype(jnp.float32)).astype(jnp.bfloat16)
    projected = dot(mixed, out_w_ref[...].reshape(chan_part, out_ref.shape[1]))
    if residual:
        projected = latents_ref[...].astype(jnp.float32) + projected
    out_ref[...] = projected.astype(out_ref.dtype)


def mix_and_project(tables, backs, latents, gate, out_w, out_depth, group, residual):
    parts = len(backs)
    owners, rows_all, chan_part = backs[0].shape
    cells, channels = latents.shape
    groups = cells // (group * WW)
    rows = rows_all // groups
    cell_block = lambda wide: pl.BlockSpec((group * WW, wide), lambda g: (g, 0))
    return pl.pallas_call(
        lambda *refs: mix_kernel(parts, residual, *refs),
        grid=(groups,),
        in_specs=[
            *[pl.BlockSpec(table.shape, lambda g: (0, 0)) for table in tables],
            *[pl.BlockSpec((owners, rows, chan_part), lambda g: (0, g, 0)) for _ in backs],
            cell_block(channels),
            cell_block(chan_part),
            pl.BlockSpec((out_w.shape[0], out_depth, channels), lambda g: (0, 0, 0)),
        ],
        out_specs=cell_block(channels),
        out_shape=jax.ShapeDtypeStruct((cells, channels), jnp.bfloat16),
        compiler_params=pltpu.CompilerParams(vmem_limit_bytes=56 * 2**20),
        name="mix_and_project",
    )(*tables, *backs, latents, gate, out_w)


MESH = pl.DeviceIdType.MESH
ANY = pl.ANY

FWD_ORDER = (2, 3, 1, 0)
BWD_ORDER = (1, 0, 2, 3)


def cas_values(length):
    position = np.arange(length)
    phase_angle = (position[:, None] * position[None, :] % length).astype(np.float32)
    phase_angle = phase_angle * np.float32(2.0 * math.pi / length)
    table = (np.cos(phase_angle) + np.sin(phase_angle)) / np.float32(math.sqrt(length))
    return table.astype(jnp.bfloat16)


def widened_values(table, copies):
    return np.kron(table.astype(np.float32), np.eye(copies, dtype=np.float32)).astype(jnp.bfloat16)


class Plan:
    def __init__(self, n, rows, channels):
        self.n = n
        self.bits = n.bit_length() - 1
        self.channels = channels
        self.lines = rows // WW
        self.band = WW // n
        self.parts = 2
        self.sub = self.band // self.parts
        self.group = TILE // self.sub
        self.groups = self.lines // self.group
        self.block = self.lines * self.sub
        self.frame = HH * self.sub
        self.width = min(256, channels)
        self.depth = channels // n


def flow_kernel(
    plan,
    latents,
    spectrum,
    value_w,
    gate_w,
    out_w,
    embed,
    ids,
    step_row,
    bands,
    bands_t,
    height,
    time,
    sent,
    planes,
    filtered,
    back,
    out,
    full,
    full_rest,
    pool_all,
    lat,
    embed_vm,
    table,
    table_t,
    stage,
    pv,
    weight,
    weight_out,
    arrived,
    residual,
    result,
    gains,
    spec,
    out_vm,
    pool_vm,
    pool_col,
    scale,
    lat_sem,
    embed_sem,
    own_sem,
    stage_sem,
    pv_sem,
    gain_sem,
    weight_sem,
    out_sem,
    misc_sem,
    arrived_sem,
    residual_sem,
    result_sem,
    ag_send,
    ag_recv,
    fwd_send,
    fwd_recv,
    bwd_send,
    bwd_recv,
):
    n, channels, sub, block = plan.n, plan.channels, plan.sub, plan.block
    lines, group, groups, width = plan.lines, plan.group, plan.groups, plan.width
    me = lax.axis_index("sp")
    local_copy = pltpu.make_async_copy

    def remote(source, target, send, recv, peer):
        return pltpu.make_async_remote_copy(
            source, target, send, recv, device_id={"sp": peer}, device_id_type=MESH
        )

    quarter = n // 4
    high, low = me // quarter, me % quarter

    def far_high(turn):
        swapped = high + 2 * (1 - 2 * (high // 2)) if turn >= 2 else high
        return swapped + (1 - 2 * (swapped % 2)) if turn % 2 else swapped

    def after(turn, j):
        return far_high(turn) * quarter + (low + j) % quarter

    def before(turn, j):
        return far_high(turn) * quarter + (low + quarter - j) % quarter

    def each_peer(body, order=(1, 0, 2, 3)):
        for turn in order:

            def one(j, carry, turn=turn):
                body(turn, j)
                return carry

            lax.fori_loop(0 if turn else 1, quarter, one, 0)

    barrier = pltpu.get_barrier_semaphore()

    def greet(turn, j):
        pl.semaphore_signal(
            barrier, inc=1, device_id={"sp": after(turn, j)}, device_id_type=MESH
        )

    each_peer(greet)

    owned = [
        local_copy(value_w, full.at[me], own_sem.at[0]),
        local_copy(gate_w, full_rest.at[me, 0], own_sem.at[1]),
        local_copy(out_w, full_rest.at[me, 1], own_sem.at[2]),
    ]
    for copy in owned:
        copy.start()
    rows = group * WW

    def lat_copy(g):
        return local_copy(
            latents.at[pl.ds(g * rows, rows), :], lat.at[pl.ds(g * rows, rows), :], lat_sem.at[g]
        )

    for g in range(groups):
        lat_copy(g).start()
    embed_in = local_copy(embed, embed_vm, embed_sem)
    embed_in.start()

    lanes = 128

    def pool_part():
        tokens = ids.shape[1]
        highs = embed_vm.shape[1] // lanes
        token = ids[...]
        upper = lax.broadcasted_iota(jnp.int32, (highs, tokens), 0) == token // lanes
        lower = lax.broadcasted_iota(jnp.int32, (lanes, tokens), 0) == token % lanes
        counts = lax.dot_general(
            upper.astype(jnp.float32).astype(jnp.bfloat16),
            lower.astype(jnp.float32).astype(jnp.bfloat16),
            (((1,), (1,)), ((), ())),
            preferred_element_type=jnp.float32,
        )
        scale[...] = counts
        embed_in.wait()

        def pool_step(i, total):
            first = pl.multiple_of(i * 8, 8)
            some = scale[pl.ds(first, 8), :]
            for k in range(8):
                column = embed_vm[:, pl.ds(pl.multiple_of((first + k) * lanes, lanes), lanes)]
                total += column.astype(jnp.float32) * some[k : k + 1, :]
            return total

        total = jnp.zeros((plan.depth, lanes), jnp.float32)
        total = lax.fori_loop(0, highs // 8, pool_step, total)
        pooled = jnp.sum(total, axis=1, keepdims=True) / tokens
        pool_vm[...] = jnp.broadcast_to(pooled, (plan.depth, lanes))
        pool_own = local_copy(pool_vm, pool_all.at[me], misc_sem)
        pool_own.start()
        pool_own.wait()

    def doubling(i):
        size = n >> (i + 1)
        peer = me + size * (1 - 2 * ((me // size) % 2))
        base = me % (2 * size)
        return size, peer, base

    gathered = (full, full_rest, pool_all)

    def gather_start(k, i):
        size, peer, base = doubling(i)
        ref = gathered[k]

        def one(j, carry):
            owner = base + 2 * size * j
            remote(ref.at[owner], ref.at[owner], ag_send.at[k, i], ag_recv.at[k, i], peer).start()
            return carry

        lax.fori_loop(0, 1 << i, one, 0)

    def gather_wait(k, i):
        _, peer, _ = doubling(i)
        some = gathered[k].at[pl.ds(0, 1 << i)]
        whole = remote(some, some, ag_send.at[k, i], ag_recv.at[k, i], peer)
        whole.wait_send()
        whole.wait_recv()

    def build_tables(p):
        wide, tall = n * group * sub, group * WW
        row = lax.broadcasted_iota(jnp.int32, (wide, n * sub), 0)
        column = lax.broadcasted_iota(jnp.int32, (wide, n * sub), 1)
        pick = (row // (group * sub)) * sub + row % sub == column
        pick = pick.astype(jnp.float32).astype(jnp.bfloat16)
        spread = dot(pick, bands[p])
        row = lax.broadcasted_iota(jnp.int32, (n * sub, wide), 0)
        column = lax.broadcasted_iota(jnp.int32, (n * sub, wide), 1)
        pick = (column // (group * sub)) * sub + column % sub == row
        pick = pick.astype(jnp.float32).astype(jnp.bfloat16)
        spread_t = dot(bands_t[p], pick)
        line = lax.broadcasted_iota(jnp.int32, (wide, WW), 0) // sub % group
        line_t = lax.broadcasted_iota(jnp.int32, (WW, wide), 1) // sub % group
        for k in range(group):
            table[:, k * WW : (k + 1) * WW] = jnp.where(line == k, spread, 0.0).astype(jnp.bfloat16)
            table_t[p, k * WW : (k + 1) * WW, :] = jnp.where(line_t == k, spread_t, 0.0).astype(
                jnp.bfloat16
            )

    def stage_copy(p, g):
        slot = g % 2
        some = pl.ds(pl.multiple_of(g * TILE, TILE), TILE)
        return local_copy(stage.at[slot], sent.at[p, :, some, :], stage_sem.at[slot])

    def fwd_copy(p, g, turn, j):
        some = pl.ds(pl.multiple_of(g * TILE, TILE), TILE)
        step = turn * quarter + j
        return remote(
            sent.at[p, after(turn, j), some, :],
            planes.at[p, me, some, :],
            fwd_send.at[p, g, step],
            fwd_recv.at[p, g, step],
            after(turn, j),
        )

    def width_group(p, g):
        if p == 0:
            lat_copy(g).wait()
        moved = dot(table[...], lat[pl.ds(pl.multiple_of(g * rows, rows), rows), :])
        stage[g % 2] = moved.reshape(n, TILE, channels).astype(jnp.bfloat16)
        stage_copy(p, g).start()

    def fwd_group(p, g):
        stage_copy(p, g).wait()
        each_peer(lambda turn, j: fwd_copy(p, g, turn, j).start(), FWD_ORDER)

    def width_groups(p, first, last):
        def one(g, carry):
            width_group(p, g)

            @pl.when(g > first)
            def _():
                fwd_group(p, g - 1)

            return carry

        lax.fori_loop(first, last, one, 0)

    build_tables(0)
    for copy in owned:
        copy.wait()
    pl.semaphore_wait(barrier, n - 1)
    gather_start(0, 0)
    gather_start(1, 0)
    middle = max(1, groups // 2)
    width_groups(0, 0, middle)
    fwd_group(0, middle - 1)
    gather_wait(0, 0)
    gather_start(0, 1)
    gather_wait(1, 0)
    gather_start(1, 1)
    width_groups(0, middle, groups)
    fwd_group(0, groups - 1)
    gather_wait(0, 1)
    gather_start(0, 2)
    build_tables(1)
    width_groups(1, 0, groups)
    fwd_group(1, groups - 1)
    gather_wait(1, 1)
    gather_start(1, 2)
    pool_part()
    gather_start(2, 0)
    for i in range(2, plan.bits):
        gather_wait(0, i)
        if i + 1 < plan.bits:
            gather_start(0, i + 1)
    gather_wait(1, 2)
    if plan.bits > 3:
        gather_start(1, 3)
    value_in = local_copy(full, weight.at[0], weight_sem.at[0])
    value_in.start()
    value_in.wait()

    def gate_part():
        rest_in = [
            local_copy(full_rest.at[:, 0], weight.at[1], weight_sem.at[0]),
            local_copy(full_rest.at[:, 1], weight_out, weight_sem.at[1]),
            local_copy(pool_all, pool_col, misc_sem),
        ]
        for copy in rest_in:
            copy.start()
        for copy in rest_in:
            copy.wait()
        column = pool_col[...].reshape(channels, lanes)
        scale_row = 1.0 + column.T[0:1, :] + step_row[...]
        chunk = min(256, lines * WW)

        def gate_step(i, carry):
            some = pl.ds(pl.multiple_of(i * chunk, chunk), chunk)
            value = dot(lat[some, :], weight[1].reshape(channels, channels))
            value = value / (1.0 + jnp.exp(-value))
            lat[some, :] = (value * scale_row).astype(jnp.bfloat16)
            return carry

        lax.fori_loop(0, lines * WW // chunk, gate_step, 0)

    def gain_copy(cb):
        slot = cb % 2
        cols = pl.ds(pl.multiple_of(cb * width, width), width)
        return local_copy(spectrum.at[:, :, :, cols], gains.at[slot], gain_sem.at[slot])

    def bwd_copy(p, g, turn, j):
        each = block if p + 1 < plan.parts else TILE
        step = turn * quarter + j
        start = pl.multiple_of(after(turn, j) * block + g * each, each)
        target = back.at[p, me, pl.ds(pl.multiple_of(g * each, each), each), :]
        return remote(
            filtered.at[p, pl.ds(start, each), :],
            target,
            bwd_send.at[p, g, step],
            bwd_recv.at[p, g, step],
            after(turn, j),
        )

    blocks = channels // width
    pieces = plan.frame // TILE

    def plane_part(p):
        def arrive(turn, j):
            source = before(turn, j)

            def one(g, carry):
                fwd_copy(p, g, turn, j).wait_recv()
                return carry

            lax.fori_loop(0, groups, one, 0)
            place = pl.ds(pl.multiple_of(source * block, block), block)
            local_copy(planes.at[p, source], pv.at[place, :], pv_sem).start()

        place = pl.ds(pl.multiple_of(me * block, block), block)
        local_copy(sent.at[p, me], pv.at[place, :], pv_sem).start()
        gain_copy(0).start()
        each_peer(arrive)
        local_copy(filtered.at[p], pv, pv_sem).wait()

        def columns(cb, carry):
            cols = pl.ds(pl.multiple_of(cb * width, width), width)
            slot = cb % 2
            gain_copy(cb).wait()

            @pl.when(cb + 1 < blocks)
            def _():
                gain_copy(cb + 1).start()

            def forward(t, inner):
                some = pl.ds(pl.multiple_of(t * plan.frame, plan.frame), plan.frame)
                w = weight[0, :, :, cols].reshape(channels, width)
                value = dot(pv[some, :], w).astype(jnp.bfloat16)
                spec[t] = dot(height[...], value).astype(jnp.bfloat16)
                return inner

            lax.fori_loop(0, TT, forward, 0, unroll=2)

            def across(i, inner):
                some = pl.ds(pl.multiple_of(i * TILE, TILE), TILE)
                one = spec[:, some, :].reshape(TT * TILE, width)
                whole = dot(time[...], one)
                each = TILE // sub
                gain = gains[
                    slot,
                    :,
                    pl.ds(pl.multiple_of(i * each, each), each),
                    p * sub : (p + 1) * sub,
                    :,
                ]
                gain = gain.reshape(TT * TILE, width).astype(jnp.float32)
                kept = (whole * gain).astype(jnp.bfloat16)
                spec[:, some, :] = dot(time[...], kept).astype(jnp.bfloat16).reshape(TT, TILE, width)
                return inner

            lax.fori_loop(0, pieces, across, 0)

            def backward(t, inner):
                some = pl.ds(pl.multiple_of(t * plan.frame, plan.frame), plan.frame)
                out_vm[some, cols] = dot(height[...], spec[t]).astype(jnp.bfloat16)
                return inner

            lax.fori_loop(0, TT, backward, 0, unroll=2)
            return carry

        lax.fori_loop(0, blocks, columns, 0)
        own = local_copy(out_vm.at[place, :], back.at[p, me], own_sem.at[0])
        whole = local_copy(out_vm, filtered.at[p], out_sem)
        own.start()
        whole.start()
        whole.wait()
        own.wait()

        def send_group(g, carry):
            each_peer(lambda turn, j: bwd_copy(p, g, turn, j).start(), BWD_ORDER)
            return carry

        lax.fori_loop(0, groups if p + 1 == plan.parts else 1, send_group, 0)

    plane_part(0)
    gather_wait(2, 0)
    gather_start(2, 1)
    for i in range(3, plan.bits):
        gather_wait(1, i)
        if i + 1 < plan.bits:
            gather_start(1, i + 1)
    plane_part(1)
    gather_wait(2, 1)
    gather_start(2, 2)
    for i in range(2, plan.bits):
        gather_wait(2, i)
        if i + 1 < plan.bits:
            gather_start(2, i + 1)
    gate_part()

    last = plan.parts - 1
    each_peer(lambda turn, j: bwd_copy(0, 0, turn, j).wait_recv())

    def residual_copy(g):
        slot = g % 2
        some = pl.ds(pl.multiple_of(g * rows, rows), rows)
        return local_copy(latents.at[some, :], residual.at[slot], residual_sem.at[slot])

    def result_copy(g):
        slot = g % 2
        some = pl.ds(pl.multiple_of(g * rows, rows), rows)
        return local_copy(result.at[slot], out.at[some, :], result_sem.at[slot])

    chunk = min(256, rows)
    residual_copy(0).start()

    def mix_group(g, carry):
        slot = g % 2
        each_peer(lambda turn, j: bwd_copy(last, g, turn, j).wait_recv())
        some = pl.ds(pl.multiple_of(g * TILE, TILE), TILE)
        inward = [
            local_copy(back.at[p, :, some, :], arrived.at[p], arrived_sem.at[p])
            for p in range(plan.parts)
        ]
        for copy in inward:
            copy.start()

        @pl.when(g + 1 < groups)
        def _():
            residual_copy(g + 1).start()

        @pl.when(g >= 2)
        def _():
            result_copy(g - 2).wait()

        residual_copy(g).wait()
        for copy in inward:
            copy.wait()

        def mix_step(i, inner):
            some = pl.ds(pl.multiple_of(i * chunk, chunk), chunk)
            cells = pl.ds(pl.multiple_of(g * rows + i * chunk, chunk), chunk)
            mix = 0.0
            for p in range(plan.parts):
                mix += dot(table_t[p, some, :], arrived[p].reshape(n * TILE, channels))
            mixed = (mix * lat[cells, :].astype(jnp.float32)).astype(jnp.bfloat16)
            projected = dot(mixed, weight_out[...].reshape(channels, channels))
            total = residual[slot, some, :].astype(jnp.float32) + projected
            result[slot, some, :] = total.astype(jnp.bfloat16)
            return inner

        lax.fori_loop(0, rows // chunk, mix_step, 0)
        result_copy(g).start()
        return carry

    lax.fori_loop(0, groups, mix_group, 0)
    for g in range(max(0, groups - 2), groups):
        result_copy(g).wait()

    for p in range(plan.parts):

        def settle(g, carry, p=p):
            each_peer(lambda turn, j: fwd_copy(p, g, turn, j).wait_send())
            return carry

        lax.fori_loop(0, groups, settle, 0)

        def settle_back(g, carry, p=p):
            each_peer(lambda turn, j: bwd_copy(p, g, turn, j).wait_send())
            return carry

        lax.fori_loop(0, groups if p == last else 1, settle_back, 0)


def flow(plan, latents, spectrum, weights, embed, ids, step_row):
    n, channels, parts = plan.n, plan.channels, plan.parts
    wide, tall = n * plan.group * plan.sub, plan.group * WW
    cells = latents.shape[0]
    plane_rows = n * plan.block
    bands = cas_values(WW).reshape(n, parts, plan.sub, WW).transpose(1, 0, 2, 3)
    bands = bands.reshape(parts, n * plan.sub, WW)
    bf, f32 = jnp.bfloat16, jnp.float32
    vmem, dma = pltpu.VMEM, pltpu.SemaphoreType.DMA
    whole = pl.BlockSpec(memory_space=vmem)
    far = pl.BlockSpec(memory_space=ANY)
    moving = (parts, n, plan.block, channels)
    highs = embed.shape[1] // 128
    outs = [
        (moving, bf),
        (moving, bf),
        ((parts, plane_rows, channels), bf),
        (moving, bf),
        ((cells, channels), bf),
        ((n, plan.depth, channels), bf),
        ((n, 2, plan.depth, channels), bf),
        ((n, plan.depth, 128), f32),
    ]
    return pl.pallas_call(
        lambda *refs: flow_kernel(plan, *refs),
        in_specs=[far, far, whole, whole, whole, far] + [whole] * 6,
        out_specs=[far] * len(outs),
        out_shape=[jax.ShapeDtypeStruct(shape, dtype) for shape, dtype in outs],
        scratch_shapes=[
            vmem((cells, channels), bf),
            vmem(embed.shape, bf),
            vmem((wide, tall), bf),
            vmem((parts, tall, wide), bf),
            vmem((2, n, TILE, channels), bf),
            vmem((plane_rows, channels), bf),
            vmem((2, n, plan.depth, channels), bf),
            vmem((n, plan.depth, channels), bf),
            vmem((parts, n, TILE, channels), bf),
            vmem((2, tall, channels), bf),
            vmem((2, tall, channels), bf),
            vmem((2, TT, HH, plan.band, plan.width), bf),
            vmem((TT, plan.frame, plan.width), bf),
            vmem((plane_rows, channels), bf),
            vmem((plan.depth, 128), f32),
            vmem((n, plan.depth, 128), f32),
            vmem((highs, 128), f32),
            dma((plan.groups,)),
            dma,
            dma((3,)),
            dma((2,)),
            dma,
            dma((2,)),
            dma((2,)),
            dma,
            dma,
            dma((parts,)),
            dma((2,)),
            dma((2,)),
            dma((3, plan.bits)),
            dma((3, plan.bits)),
            dma((parts, plan.groups, n)),
            dma((parts, plan.groups, n)),
            dma((parts, plan.groups, n)),
            dma((parts, plan.groups, n)),
        ],
        compiler_params=pltpu.CompilerParams(
            collective_id=0, has_side_effects=True, vmem_limit_bytes=60 * 2**20
        ),
        name="flow",
    )(
        latents,
        spectrum,
        *weights,
        embed,
        ids,
        step_row,
        bands,
        bands.transpose(0, 2, 1),
        widened_values(cas_values(HH), plan.sub),
        widened_values(cas_values(TT), TILE),
    )


def streamed(latents, spectrum, w_value, w_gate, w_out, embed_table, prompt_ids, noise_step):
    rows, channels = latents.shape
    plan = Plan(lax.axis_size("sp"), rows, channels)
    channel = jnp.arange(channels, dtype=jnp.int32)
    step_row = step_embedding(noise_step, channel, C)[None, :]
    outs = flow(
        plan,
        latents,
        spectrum,
        (w_value, w_gate, w_out),
        embed_table,
        prompt_ids[None, :],
        step_row,
    )
    return outs[4]


def fits(mesh):
    n = mesh.shape["sp"]
    alone = mesh.shape["grp"] == 1 and mesh.shape["ch"] == 1
    band = WW // n
    return alone and n >= 8 and n & (n - 1) == 0 and band >= 2 and TT * HH // n * band >= 2 * TILE


def exchange(blocks):
    return lax.all_to_all(blocks, "sp", split_axis=0, concat_axis=0, tiled=True)


def local(latents, spectrum, w_value, w_gate, w_out, embed_table, prompt_ids, noise_step):
    row_count, channels = latents.shape
    chan_part = w_value.shape[1]
    owners = lax.axis_size("sp")
    splits = lax.axis_size("ch")
    lines = row_count // WW
    band = WW // owners
    group = min(lines, max(1, TILE // band))

    parts = 2 if band % 2 == 0 else 1
    sub = band // parts

    table = cas_table(WW).reshape(owners, parts, 1, sub, 1, WW)
    same_line = jnp.eye(group, dtype=jnp.bfloat16).reshape(1, group, 1, group, 1)
    width_tables = [
        (table[:, part] * same_line).reshape(owners * group * sub, group * WW)
        for part in range(parts)
    ]
    height_table = widened(cas_table(HH), sub)
    time_table = widened(cas_table(TT), TILE)
    gains = spectrum.reshape(TT, HH, parts, sub, chan_part)

    full_value = lax.all_gather(w_value, "sp", axis=0)

    full_gate = lax.all_gather(w_gate, "sp", axis=0)
    local_pool = jnp.mean(jnp.take(embed_table, prompt_ids, axis=1).astype(jnp.float32), axis=1)
    offset = lax.axis_index("ch") * chan_part
    depth = w_out.shape[0]
    if splits == 1:
        first = local_pool.astype(jnp.bfloat16)
        rest = local_pool - first.astype(jnp.float32)
        second = rest.astype(jnp.bfloat16)
        third = (rest - second.astype(jnp.float32)).astype(jnp.bfloat16)
        terms = jnp.stack([first, second, third])
        terms = jnp.pad(terms, ((0, TILE - 3), (0, channels - terms.shape[1])))
        full_out = lax.all_gather(jnp.concatenate([w_out, terms], axis=0), "sp", axis=0)
    else:
        pooled_all = lax.all_gather(local_pool, ("sp", "ch"), axis=0, tiled=True)
        pooled = lax.dynamic_slice_in_dim(pooled_all, offset, chan_part)
        rows_out = lax.all_gather(w_out, "sp", axis=0, tiled=True)
        full_out = lax.dynamic_slice_in_dim(rows_out, offset, chan_part, 0)[None]
        depth = chan_part

    planes, backs = [], []
    for part in range(parts):
        sent = width_forward(width_tables[part], latents, owners, lines, sub, group)
        if planes:
            sent, planes[-1], full_value = lax.optimization_barrier((sent, planes[-1], full_value))
        planes.append(exchange(sent))
    for part in range(parts):
        filtered = plane_filter(
            height_table,
            time_table,
            planes[part].reshape(TT * HH * sub, channels),
            full_value,
            gains[:, :, part].reshape(TT, HH * sub, chan_part),
            sub,
        ).reshape(owners, lines * sub, chan_part)
        if backs:
            filtered, backs[-1], full_gate = lax.optimization_barrier(
                (filtered, backs[-1], full_gate)
            )
        elif parts > 1:
            filtered, planes[-1], full_out = lax.optimization_barrier(
                (filtered, planes[-1], full_out)
            )
        backs.append(exchange(filtered))

    if splits == 1:
        pooled = full_out[:, depth : depth + 3, : local_pool.shape[0]].astype(jnp.float32)
        pooled = jnp.sum(pooled, axis=1).reshape(chan_part)
    channel = offset + jnp.arange(chan_part, dtype=jnp.int32)
    modulation = 1.0 + pooled + step_embedding(noise_step, channel, C)

    gate = gate_rows(latents, full_gate, modulation[None, :])
    mixed = mix_and_project(
        [width_table.T for width_table in width_tables],
        backs,
        latents,
        gate,
        full_out,
        depth,
        group,
        splits == 1,
    )
    if splits == 1:
        return mixed
    half_rows = row_count // splits
    summed = lax.psum_scatter(mixed, "ch", scatter_dimension=0, tiled=True).astype(jnp.float32)
    residual = lax.dynamic_slice_in_dim(latents, lax.axis_index("ch") * half_rows, half_rows, 0)
    return (residual.astype(jnp.float32) + summed).astype(jnp.bfloat16)


def solution(mesh):
    placed = (
        P(("grp", "sp"), None),
        P(None, None, "sp", "ch"),
        P("sp", "ch"),
        P("sp", "ch"),
        P("sp", None),
        P(("sp", "ch"), None),
        P("grp"),
        P("grp"),
    )
    return jax.shard_map(
        streamed if fits(mesh) else local,
        mesh=mesh, in_specs=placed, out_specs=P(("grp", "sp", "ch"), None), check_vma=False
    )
```

```python
import math

import jax
import jax.numpy as jnp
import numpy as np
from jax import lax
from jax.experimental import pallas as pl
from jax.experimental.pallas import tpu as pltpu
from jax.sharding import PartitionSpec as P

TT = 16
HH = 64
WW = 128
C = 1024

TILE = 16


def cas_table(length):
    position = jnp.arange(length, dtype=jnp.int32)
    product = position[:, None] * position[None, :] % length
    phase_angle = product.astype(jnp.float32) * (2.0 * math.pi / length)
    return ((jnp.cos(phase_angle) + jnp.sin(phase_angle)) / math.sqrt(length)).astype(jnp.bfloat16)


def step_embedding(noise_step, channel, channels):
    half_count = channels // 2
    lower_half = channel < half_count
    position = jnp.where(lower_half, channel, channel - half_count).astype(jnp.float32)
    frequency = jnp.exp(-math.log(10000.0) * position / half_count)
    phase_angle = noise_step[0].astype(jnp.float32) * frequency
    return jnp.where(lower_half, jnp.sin(phase_angle), jnp.cos(phase_angle))


def widened(table, copies):
    length = table.shape[0]
    inner = jnp.eye(copies, dtype=table.dtype)
    both = table[:, None, :, None] * inner[None, :, None, :]
    return both.reshape(length * copies, length * copies)


def dot(left, right):
    return jnp.dot(left, right, preferred_element_type=jnp.float32)


def width_kernel(table_ref, latents_ref, out_ref):
    owners, rows, channels = out_ref.shape
    moved = dot(table_ref[...], latents_ref[...])
    out_ref[...] = moved.reshape(owners, rows, channels).astype(out_ref.dtype)


def width_forward(table, latents, owners, lines, band, group):
    channels = latents.shape[1]
    rows = group * WW
    cells = lines * WW
    return pl.pallas_call(
        width_kernel,
        grid=(lines // group,),
        in_specs=[
            pl.BlockSpec(table.shape, lambda g: (0, 0)),
            pl.BlockSpec((rows, channels), lambda g: (g, 0)),
        ],
        out_specs=pl.BlockSpec((owners, group * band, channels), lambda g: (0, g, 0)),
        out_shape=jax.ShapeDtypeStruct((owners, lines * band, channels), jnp.bfloat16),
        compiler_params=pltpu.CompilerParams(vmem_limit_bytes=48 * 2**20),
        cost_estimate=pl.CostEstimate(
            flops=2 * cells * table.shape[0] * channels,
            bytes_accessed=4 * cells * channels,
            transcendentals=0,
        ),
        name="width_forward",
    )(table, latents)


def plane_kernel(band, height_ref, time_ref, planes_ref, weight_ref, spectrum_ref, out_ref, spec):
    per_frame = HH * band
    width = out_ref.shape[1]
    pieces = per_frame // TILE
    weight = weight_ref[...].reshape(planes_ref.shape[1], width)

    def forward(t, carry):
        rows = pl.ds(pl.multiple_of(t * per_frame, per_frame), per_frame)
        value = dot(planes_ref[rows, :], weight).astype(jnp.bfloat16)
        spec[t] = dot(height_ref[...], value).astype(jnp.bfloat16)
        return carry

    lax.fori_loop(0, TT, forward, 0, unroll=4)

    def across(p, carry):
        rows = pl.ds(pl.multiple_of(p * TILE, TILE), TILE)
        block = spec[:, rows, :].reshape(TT * TILE, width)
        full = dot(time_ref[...], block)
        gain = spectrum_ref[:, rows, :].reshape(TT * TILE, width).astype(jnp.float32)
        filtered = (full * gain).astype(jnp.bfloat16)
        back = dot(time_ref[...], filtered).astype(jnp.bfloat16)
        spec[:, rows, :] = back.reshape(TT, TILE, width)
        return carry

    lax.fori_loop(0, pieces, across, 0, unroll=4)

    def backward(t, carry):
        rows = pl.ds(pl.multiple_of(t * per_frame, per_frame), per_frame)
        out_ref[rows, :] = dot(height_ref[...], spec[t]).astype(jnp.bfloat16)
        return carry

    lax.fori_loop(0, TT, backward, 0, unroll=4)


def plane_filter(height, time, planes, weight, spectrum, band):
    cells, channels = planes.shape
    shards, depth, chan_part = weight.shape
    width = min(256, chan_part)
    per_frame = HH * band
    return pl.pallas_call(
        lambda *refs: plane_kernel(band, *refs),
        grid=(chan_part // width,),
        in_specs=[
            pl.BlockSpec(height.shape, lambda g: (0, 0)),
            pl.BlockSpec(time.shape, lambda g: (0, 0)),
            pl.BlockSpec((cells, channels), lambda g: (0, 0)),
            pl.BlockSpec((shards, depth, width), lambda g: (0, 0, g)),
            pl.BlockSpec((TT, per_frame, width), lambda g: (0, 0, g)),
        ],
        out_specs=pl.BlockSpec((cells, width), lambda g: (0, g)),
        out_shape=jax.ShapeDtypeStruct((cells, chan_part), jnp.bfloat16),
        scratch_shapes=[pltpu.VMEM((TT, per_frame, width), jnp.bfloat16)],
        cost_estimate=pl.CostEstimate(
            flops=2 * cells * chan_part * (channels + 1024),
            bytes_accessed=2 * cells * (channels + 2 * chan_part),
            transcendentals=0,
        ),
        compiler_params=pltpu.CompilerParams(vmem_limit_bytes=56 * 2**20),
        name="plane_filter",
    )(height, time, planes, weight, spectrum)


def gate_kernel(latents_ref, gate_ref, scale_ref, out_ref):
    gate = dot(latents_ref[...], gate_ref[...].reshape(latents_ref.shape[1], out_ref.shape[1]))
    gate = gate / (1.0 + jnp.exp(-gate))
    out_ref[...] = (gate * scale_ref[...]).astype(out_ref.dtype)


def gate_rows(latents, gate_w, scale):
    cells, channels = latents.shape
    chan_part = gate_w.shape[2]
    rows = min(512, cells)
    return pl.pallas_call(
        gate_kernel,
        grid=(cells // rows,),
        in_specs=[
            pl.BlockSpec((rows, channels), lambda g: (g, 0)),
            pl.BlockSpec(gate_w.shape, lambda g: (0, 0, 0)),
            pl.BlockSpec((1, chan_part), lambda g: (0, 0)),
        ],
        out_specs=pl.BlockSpec((rows, chan_part), lambda g: (g, 0)),
        out_shape=jax.ShapeDtypeStruct((cells, chan_part), jnp.bfloat16),
        compiler_params=pltpu.CompilerParams(vmem_limit_bytes=48 * 2**20),
        cost_estimate=pl.CostEstimate(
            flops=2 * cells * channels * chan_part,
            bytes_accessed=2 * cells * (channels + chan_part),
            transcendentals=cells * chan_part,
        ),
        name="gate_rows",
    )(latents, gate_w, scale)


def mix_kernel(parts, residual, *refs):
    tables, backs = refs[:parts], refs[parts : 2 * parts]
    latents_ref, gate_ref, out_w_ref, out_ref = refs[2 * parts :]
    owners, rows, chan_part = backs[0].shape
    mix = dot(tables[0][...], backs[0][...].reshape(owners * rows, chan_part))
    for table_ref, back_ref in zip(tables[1:], backs[1:]):
        mix += dot(table_ref[...], back_ref[...].reshape(owners * rows, chan_part))
    mixed = (mix * gate_ref[...].astype(jnp.float32)).astype(jnp.bfloat16)
    projected = dot(mixed, out_w_ref[...].reshape(chan_part, out_ref.shape[1]))
    if residual:
        projected = latents_ref[...].astype(jnp.float32) + projected
    out_ref[...] = projected.astype(out_ref.dtype)


def mix_and_project(tables, backs, latents, gate, out_w, out_depth, group, residual):
    parts = len(backs)
    owners, rows_all, chan_part = backs[0].shape
    cells, channels = latents.shape
    groups = cells // (group * WW)
    rows = rows_all // groups
    cell_block = lambda wide: pl.BlockSpec((group * WW, wide), lambda g: (g, 0))
    return pl.pallas_call(
        lambda *refs: mix_kernel(parts, residual, *refs),
        grid=(groups,),
        in_specs=[
            *[pl.BlockSpec(table.shape, lambda g: (0, 0)) for table in tables],
            *[pl.BlockSpec((owners, rows, chan_part), lambda g: (0, g, 0)) for _ in backs],
            cell_block(channels),
            cell_block(chan_part),
            pl.BlockSpec((out_w.shape[0], out_depth, channels), lambda g: (0, 0, 0)),
        ],
        out_specs=cell_block(channels),
        out_shape=jax.ShapeDtypeStruct((cells, channels), jnp.bfloat16),
        compiler_params=pltpu.CompilerParams(vmem_limit_bytes=56 * 2**20),
        name="mix_and_project",
    )(*tables, *backs, latents, gate, out_w)


MESH = pl.DeviceIdType.MESH
ANY = pl.ANY

FWD_TURNS = (1, 2, 0, 3)
BWD_TURNS = (1, 2, 0, 3)


def cas_values(length):
    position = np.arange(length)
    phase_angle = (position[:, None] * position[None, :] % length).astype(np.float32)
    phase_angle = phase_angle * np.float32(2.0 * math.pi / length)
    table = (np.cos(phase_angle) + np.sin(phase_angle)) / np.float32(math.sqrt(length))
    return table.astype(jnp.bfloat16)


def widened_values(table, copies):
    return np.kron(table.astype(np.float32), np.eye(copies, dtype=np.float32)).astype(jnp.bfloat16)


class Plan:
    def __init__(self, n, rows, channels):
        self.n = n
        self.bits = n.bit_length() - 1
        self.channels = channels
        self.lines = rows // WW
        self.band = WW // n
        self.parts = 2
        self.sub = self.band // self.parts
        self.group = TILE // self.sub
        self.groups = self.lines // self.group
        self.block = self.lines * self.sub
        self.frame = HH * self.sub
        self.width = min(256, channels)
        self.depth = channels // n


def flow_kernel(
    plan,
    latents,
    spectrum,
    value_w,
    gate_w,
    out_w,
    embed,
    ids_far,
    step_far,
    bands_far,
    bands_t_far,
    height_far,
    time_far,
    sent,
    planes,
    filtered,
    back,
    out,
    full,
    full_rest,
    pool_all,
    tables_out,
    gate_out,
    lat,
    held,
    ids,
    step_row,
    bands,
    bands_t,
    height,
    time,
    embed_vm,
    table,
    table_t,
    stage,
    pv,
    weight,
    weight_out,
    arrived,
    residual,
    result,
    gains,
    spec,
    out_vm,
    pool_vm,
    pool_col,
    scale,
    lat_sem,
    embed_sem,
    own_sem,
    stage_sem,
    pv_sem,
    gain_sem,
    weight_sem,
    out_sem,
    misc_sem,
    small_sem,
    tail_sem,
    arrived_sem,
    residual_sem,
    result_sem,
    first_send,
    first_recv,
    ag_send,
    ag_recv,
    fwd_send,
    fwd_recv,
    bwd_send,
    bwd_recv,
):
    n, channels, sub, block = plan.n, plan.channels, plan.sub, plan.block
    lines, group, groups, width = plan.lines, plan.group, plan.groups, plan.width
    me = lax.axis_index("sp")
    local_copy = pltpu.make_async_copy

    def remote(source, target, send, recv, peer):
        return pltpu.make_async_remote_copy(
            source, target, send, recv, device_id={"sp": peer}, device_id_type=MESH
        )

    flips = [(1 << b) * (1 - 2 * lax.rem(lax.div(me, 1 << b), 2)) for b in range(plan.bits)]

    def paired(mask):
        peer = me
        for b in range(plan.bits):
            peer += flips[b] * lax.rem(lax.div(mask, 1 << b), 2)
        return peer

    def each_mask(body):
        def one(mask, carry):
            body(mask)
            return carry

        lax.fori_loop(1, n, one, 0)

    quarter = n // 4
    chips = quarter // 2
    core = lax.rem(me, 2)

    def each_peer(body, turns):
        def one(step, carry):
            for i, turn in enumerate(turns):
                chip = lax.rem(step + i, chips)
                chip = chip + core * (chips - 1 - 2 * chip)
                mask = turn * quarter + chip * 2 + lax.div(step, chips)

                if turn:
                    body(mask)
                else:

                    @pl.when(mask > 0)
                    def _(mask=mask):
                        body(mask)

            return carry

        lax.fori_loop(0, quarter, one, 0)

    barrier = pltpu.get_barrier_semaphore()

    def greet(mask):
        pl.semaphore_signal(barrier, inc=1, device_id={"sp": paired(mask)}, device_id_type=MESH)

    each_mask(greet)

    small = [
        local_copy(source, target, small_sem.at[i])
        for i, (source, target) in enumerate(
            (
                (bands_far, bands),
                (bands_t_far, bands_t),
                (ids_far, ids),
                (height_far, height),
                (time_far, time),
                (step_far, step_row),
            )
        )
    ]
    small[0].start()
    small[1].start()
    rows = group * WW

    def lat_copy(g):
        return local_copy(
            latents.at[pl.ds(g * rows, rows), :], lat.at[pl.ds(g * rows, rows), :], lat_sem.at[g]
        )

    for g in range(groups):
        lat_copy(g).start()
    shards = (
        (value_w, full.at[me]),
        (gate_w, full_rest.at[me, 0]),
        (out_w, full_rest.at[me, 1]),
    )
    shards_in = [local_copy(w, held.at[i], own_sem.at[i]) for i, (w, _) in enumerate(shards)]
    owned = [local_copy(held.at[i], place, own_sem.at[i]) for i, (_, place) in enumerate(shards)]
    embed_in = local_copy(embed, embed_vm, embed_sem)
    for copy in (*shards_in, *small[2:], embed_in):
        copy.start()

    lanes = 128

    def pool_part():
        small[2].wait()
        tokens = ids.shape[1]
        highs = embed_vm.shape[1] // lanes
        token = ids[...]
        upper = lax.broadcasted_iota(jnp.int32, (highs, tokens), 0) == token // lanes
        lower = lax.broadcasted_iota(jnp.int32, (lanes, tokens), 0) == token % lanes
        counts = lax.dot_general(
            upper.astype(jnp.float32).astype(jnp.bfloat16),
            lower.astype(jnp.float32).astype(jnp.bfloat16),
            (((1,), (1,)), ((), ())),
            preferred_element_type=jnp.float32,
        )
        scale[...] = counts
        embed_in.wait()

        def pool_step(i, total):
            first = pl.multiple_of(i * 8, 8)
            some = scale[pl.ds(first, 8), :]
            for k in range(8):
                column = embed_vm[:, pl.ds(pl.multiple_of((first + k) * lanes, lanes), lanes)]
                total += column.astype(jnp.float32) * some[k : k + 1, :]
            return total

        total = jnp.zeros((plan.depth, lanes), jnp.float32)
        total = lax.fori_loop(0, highs // 8, pool_step, total)
        pooled = jnp.sum(total, axis=1, keepdims=True) / tokens
        pool_vm[...] = jnp.broadcast_to(pooled, (plan.depth, lanes))
        pool_own = local_copy(pool_vm, pool_all.at[me], misc_sem)
        pool_own.start()
        pool_own.wait()

    def doubling(i):
        size = n >> (i + 1)
        peer = me + flips[plan.bits - 1 - i]
        base = lax.rem(me, 2 * size)
        return size, peer, base

    gathered = (full, full_rest, pool_all)

    def gather_start(k, i):
        size, peer, base = doubling(i)
        ref = gathered[k]

        def one(j, carry):
            owner = base + 2 * size * j
            remote(ref.at[owner], ref.at[owner], ag_send.at[k, i], ag_recv.at[k, i], peer).start()
            return carry

        lax.fori_loop(0, 1 << i, one, 0)

    def gather_first():
        _, peer, _ = doubling(0)
        for i, (w, place) in enumerate(shards):
            remote(w, place, first_send.at[i], first_recv.at[i], peer).start()

    def gather_first_wait(i):
        _, peer, _ = doubling(0)
        w, place = shards[i]
        copy = remote(w, place, first_send.at[i], first_recv.at[i], peer)
        copy.wait_send()
        copy.wait_recv()
        owned[i].wait()

    def gather_wait(k, i):
        _, peer, _ = doubling(i)
        some = gathered[k].at[pl.ds(0, 1 << i)]
        whole = remote(some, some, ag_send.at[k, i], ag_recv.at[k, i], peer)
        whole.wait_send()
        whole.wait_recv()

    def build_tables(p):
        wide, tall = n * group * sub, group * WW
        row = lax.broadcasted_iota(jnp.int32, (wide, n * sub), 0)
        column = lax.broadcasted_iota(jnp.int32, (wide, n * sub), 1)
        pick = (row // (group * sub)) * sub + row % sub == column
        pick = pick.astype(jnp.float32).astype(jnp.bfloat16)
        spread = dot(pick, bands[p])
        row = lax.broadcasted_iota(jnp.int32, (n * sub, wide), 0)
        column = lax.broadcasted_iota(jnp.int32, (n * sub, wide), 1)
        pick = (column // (group * sub)) * sub + column % sub == row
        pick = pick.astype(jnp.float32).astype(jnp.bfloat16)
        spread_t = dot(bands_t[p], pick)
        line = lax.broadcasted_iota(jnp.int32, (wide, WW), 0) // sub % group
        line_t = lax.broadcasted_iota(jnp.int32, (WW, wide), 1) // sub % group
        for k in range(group):
            table[:, k * WW : (k + 1) * WW] = jnp.where(line == k, spread, 0.0).astype(jnp.bfloat16)
            table_t[p, k * WW : (k + 1) * WW, :] = jnp.where(line_t == k, spread_t, 0.0).astype(
                jnp.bfloat16
            )

    def stage_copy(p, g):
        slot = g % 2
        some = pl.ds(pl.multiple_of(g * TILE, TILE), TILE)
        return local_copy(stage.at[slot], sent.at[p, :, some, :], stage_sem.at[slot])

    last = plan.parts - 1
    fwd_spans = [[(0, groups)] for _ in range(plan.parts)]
    fwd_spans[0] = [(0, 1), (1, groups)]
    bwd_spans = [[(0, groups)] for _ in range(plan.parts)]
    cuts = list(range(groups + 1))
    bwd_spans[last] = list(zip(cuts, cuts[1:]))

    def fwd_copy(p, k, mask):
        first, end = fwd_spans[p][k]
        some = pl.ds(first * TILE, (end - first) * TILE)
        peer = paired(mask)
        return remote(
            sent.at[p, peer, some, :],
            planes.at[p, me, some, :],
            fwd_send.at[p, k, mask],
            fwd_recv.at[p, k, mask],
            peer,
        )

    def width_group(p, g):
        if p == 0:
            lat_copy(g).wait()
        moved = dot(table[...], lat[pl.ds(pl.multiple_of(g * rows, rows), rows), :])
        stage[g % 2] = moved.reshape(n, TILE, channels).astype(jnp.bfloat16)
        stage_copy(p, g).start()

    def fwd_start(p, k):
        each_peer(lambda mask: fwd_copy(p, k, mask).start(), FWD_TURNS)

    def width_groups(p, first, end):
        def one(g, carry):
            @pl.when(g > first)
            def _():
                stage_copy(p, g - 1).wait()

            width_group(p, g)
            return carry

        lax.fori_loop(first, end, one, 0)
        stage_copy(p, end - 1).wait()

    small[0].wait()
    small[1].wait()
    build_tables(0)
    for i in range(3):
        shards_in[i].wait()
        owned[i].start()
    pl.semaphore_wait(barrier, n - 1)
    gather_first()
    width_groups(0, 0, 1)
    fwd_start(0, 0)
    width_groups(0, 1, groups)
    gather_first_wait(0)
    gather_start(0, 1)
    gather_first_wait(1)
    gather_first_wait(2)
    gather_start(1, 1)
    fwd_start(0, 1)
    gather_wait(0, 1)
    gather_start(0, 2)
    build_tables(1)
    width_groups(1, 0, groups)
    fwd_start(1, 0)
    gather_wait(1, 1)
    gather_start(1, 2)
    pool_part()
    gather_start(2, 0)
    for i in range(2, plan.bits):
        gather_wait(0, i)
        if i + 1 < plan.bits:
            gather_start(0, i + 1)
    gather_wait(1, 2)
    if plan.bits > 3:
        gather_start(1, 3)
    value_in = local_copy(full, weight.at[0], weight_sem.at[0])
    value_in.start()
    value_in.wait()
    small[3].wait()
    small[4].wait()

    def gate_part():
        rest_in = [
            local_copy(full_rest.at[:, 0], weight.at[1], weight_sem.at[0]),
            local_copy(full_rest.at[:, 1], weight_out, weight_sem.at[1]),
            local_copy(pool_all, pool_col, misc_sem),
        ]
        for copy in rest_in:
            copy.start()
        for copy in rest_in:
            copy.wait()
        small[5].wait()
        column = pool_col[...].reshape(channels, lanes)
        scale_row = 1.0 + column.T[0:1, :] + step_row[...]
        chunk = min(256, lines * WW)

        def gate_step(i, carry):
            some = pl.ds(pl.multiple_of(i * chunk, chunk), chunk)
            value = dot(lat[some, :], weight[1].reshape(channels, channels))
            value = value / (1.0 + jnp.exp(-value))
            lat[some, :] = (value * scale_row).astype(jnp.bfloat16)
            return carry

        lax.fori_loop(0, lines * WW // chunk, gate_step, 0)

    def gain_copy(cb):
        slot = cb % 2
        cols = pl.ds(pl.multiple_of(cb * width, width), width)
        return local_copy(spectrum.at[:, :, :, cols], gains.at[slot], gain_sem.at[slot])

    def bwd_copy(p, k, mask):
        first, end = bwd_spans[p][k]
        count = (end - first) * TILE
        peer = paired(mask)
        start = pl.multiple_of(peer * block + first * TILE, TILE)
        return remote(
            filtered.at[p, pl.ds(start, count), :],
            back.at[p, me, pl.ds(first * TILE, count), :],
            bwd_send.at[p, k, mask],
            bwd_recv.at[p, k, mask],
            peer,
        )

    blocks = channels // width
    pieces = plan.frame // TILE

    def plane_part(p):
        def arrive(mask):
            source = paired(mask)

            for k in range(len(fwd_spans[p])):
                fwd_copy(p, k, mask).wait_recv()
            place = pl.ds(pl.multiple_of(source * block, block), block)
            local_copy(planes.at[p, source], pv.at[place, :], pv_sem).start()

        place = pl.ds(pl.multiple_of(me * block, block), block)
        local_copy(sent.at[p, me], pv.at[place, :], pv_sem).start()
        gain_copy(0).start()
        each_mask(arrive)
        local_copy(filtered.at[p], pv, pv_sem).wait()

        def columns(cb, carry):
            cols = pl.ds(pl.multiple_of(cb * width, width), width)
            slot = cb % 2
            gain_copy(cb).wait()

            @pl.when(cb + 1 < blocks)
            def _():
                gain_copy(cb + 1).start()

            def forward(t, inner):
                some = pl.ds(pl.multiple_of(t * plan.frame, plan.frame), plan.frame)
                w = weight[0, :, :, cols].reshape(channels, width)
                value = dot(pv[some, :], w).astype(jnp.bfloat16)
                spec[t] = dot(height[...], value).astype(jnp.bfloat16)
                return inner

            lax.fori_loop(0, TT, forward, 0, unroll=2)

            def across(i, inner):
                some = pl.ds(pl.multiple_of(i * TILE, TILE), TILE)
                one = spec[:, some, :].reshape(TT * TILE, width)
                whole = dot(time[...], one)
                each = TILE // sub
                gain = gains[
                    slot,
                    :,
                    pl.ds(pl.multiple_of(i * each, each), each),
                    p * sub : (p + 1) * sub,
                    :,
                ]
                gain = gain.reshape(TT * TILE, width).astype(jnp.float32)
                kept = (whole * gain).astype(jnp.bfloat16)
                spec[:, some, :] = dot(time[...], kept).astype(jnp.bfloat16).reshape(TT, TILE, width)
                return inner

            lax.fori_loop(0, pieces, across, 0)

            def backward(t, inner):
                some = pl.ds(pl.multiple_of(t * plan.frame, plan.frame), plan.frame)
                out_vm[some, cols] = dot(height[...], spec[t]).astype(jnp.bfloat16)
                return inner

            lax.fori_loop(0, TT, backward, 0, unroll=2)
            return carry

        lax.fori_loop(0, blocks, columns, 0)
        own = local_copy(out_vm.at[place, :], back.at[p, me], own_sem.at[0])
        whole = local_copy(out_vm, filtered.at[p], out_sem)
        own.start()
        whole.start()
        whole.wait()
        own.wait()

        for k in range(len(bwd_spans[p])):
            each_peer(lambda mask, k=k: bwd_copy(p, k, mask).start(), BWD_TURNS)

    plane_part(0)
    gather_wait(2, 0)
    gather_start(2, 1)
    for i in range(3, plan.bits):
        gather_wait(1, i)
        if i + 1 < plan.bits:
            gather_start(1, i + 1)
    plane_part(1)
    gather_wait(2, 1)
    gather_start(2, 2)
    for i in range(2, plan.bits):
        gather_wait(2, i)
        if i + 1 < plan.bits:
            gather_start(2, i + 1)
    gate_part()

    tail = [
        local_copy(table_t, tables_out, tail_sem.at[0]),
        local_copy(lat.at[pl.ds((groups - 1) * rows, rows), :], gate_out, tail_sem.at[1]),
    ]
    for copy in tail:
        copy.start()

    for p in range(last):
        each_mask(lambda mask, p=p: bwd_copy(p, 0, mask).wait_recv())

    def residual_copy(g):
        slot = g % 2
        some = pl.ds(pl.multiple_of(g * rows, rows), rows)
        return local_copy(latents.at[some, :], residual.at[slot], residual_sem.at[slot])

    def result_copy(g):
        slot = g % 2
        some = pl.ds(pl.multiple_of(g * rows, rows), rows)
        return local_copy(result.at[slot], out.at[some, :], result_sem.at[slot])

    chunk = min(256, rows)
    residual_copy(0).start()

    def mix_group(g, carry):
        slot = g % 2
        some = pl.ds(pl.multiple_of(g * TILE, TILE), TILE)
        inward = [
            local_copy(back.at[p, :, some, :], arrived.at[p], arrived_sem.at[p])
            for p in range(plan.parts)
        ]
        for copy in inward:
            copy.start()

        @pl.when(g + 2 < groups)
        def _():
            residual_copy(g + 1).start()

        @pl.when(g >= 2)
        def _():
            result_copy(g - 2).wait()

        residual_copy(g).wait()
        for copy in inward:
            copy.wait()

        def mix_step(i, inner):
            some = pl.ds(pl.multiple_of(i * chunk, chunk), chunk)
            cells = pl.ds(pl.multiple_of(g * rows + i * chunk, chunk), chunk)
            mix = 0.0
            for p in range(plan.parts):
                mix += dot(table_t[p, some, :], arrived[p].reshape(n * TILE, channels))
            mixed = (mix * lat[cells, :].astype(jnp.float32)).astype(jnp.bfloat16)
            projected = dot(mixed, weight_out[...].reshape(channels, channels))
            total = residual[slot, some, :].astype(jnp.float32) + projected
            result[slot, some, :] = total.astype(jnp.bfloat16)
            return inner

        lax.fori_loop(0, rows // chunk, mix_step, 0)
        result_copy(g).start()
        return carry

    for k, (first, end) in enumerate(bwd_spans[last][:-1]):
        each_mask(lambda mask, k=k: bwd_copy(last, k, mask).wait_recv())
        lax.fori_loop(first, end, mix_group, 0)
    for g in range(max(0, groups - 3), groups - 1):
        result_copy(g).wait()
    for copy in tail:
        copy.wait()

    for p in range(plan.parts):
        for k in range(len(fwd_spans[p])):
            each_mask(lambda mask, p=p, k=k: fwd_copy(p, k, mask).wait_send())
        for k in range(len(bwd_spans[p])):
            each_mask(lambda mask, p=p, k=k: bwd_copy(p, k, mask).wait_send())
    each_mask(lambda mask: bwd_copy(last, len(bwd_spans[last]) - 1, mask).wait_recv())


def flow(plan, latents, spectrum, weights, embed, ids, step_row):
    n, channels, parts = plan.n, plan.channels, plan.parts
    wide, tall = n * plan.group * plan.sub, plan.group * WW
    cells = latents.shape[0]
    plane_rows = n * plan.block
    bands = cas_values(WW).reshape(n, parts, plan.sub, WW).transpose(1, 0, 2, 3)
    bands = bands.reshape(parts, n * plan.sub, WW)
    bf, f32 = jnp.bfloat16, jnp.float32
    vmem, dma = pltpu.VMEM, pltpu.SemaphoreType.DMA
    far = pl.BlockSpec(memory_space=ANY)
    moving = (parts, n, plan.block, channels)
    highs = embed.shape[1] // 128
    outs = [
        (moving, bf),
        (moving, bf),
        ((parts, plane_rows, channels), bf),
        (moving, bf),
        ((cells - tall, channels), bf),
        ((n, plan.depth, channels), bf),
        ((n, 2, plan.depth, channels), bf),
        ((n, plan.depth, 128), f32),
        ((parts, tall, wide), bf),
        ((tall, channels), bf),
    ]
    return pl.pallas_call(
        lambda *refs: flow_kernel(plan, *refs),
        in_specs=[far] * 12,
        out_specs=[far] * len(outs),
        out_shape=[jax.ShapeDtypeStruct(shape, dtype) for shape, dtype in outs],
        scratch_shapes=[
            vmem((cells, channels), bf),
            vmem((3, plan.depth, channels), bf),
            vmem(ids.shape, jnp.int32),
            vmem(step_row.shape, f32),
            vmem(bands.shape, bf),
            vmem((parts, WW, n * plan.sub), bf),
            vmem((plan.frame, plan.frame), bf),
            vmem((TT * TILE, TT * TILE), bf),
            vmem(embed.shape, bf),
            vmem((wide, tall), bf),
            vmem((parts, tall, wide), bf),
            vmem((2, n, TILE, channels), bf),
            vmem((plane_rows, channels), bf),
            vmem((2, n, plan.depth, channels), bf),
            vmem((n, plan.depth, channels), bf),
            vmem((parts, n, TILE, channels), bf),
            vmem((2, tall, channels), bf),
            vmem((2, tall, channels), bf),
            vmem((2, TT, HH, plan.band, plan.width), bf),
            vmem((TT, plan.frame, plan.width), bf),
            vmem((plane_rows, channels), bf),
            vmem((plan.depth, 128), f32),
            vmem((n, plan.depth, 128), f32),
            vmem((highs, 128), f32),
            dma((plan.groups,)),
            dma,
            dma((3,)),
            dma((2,)),
            dma,
            dma((2,)),
            dma((2,)),
            dma,
            dma,
            dma((6,)),
            dma((2,)),
            dma((parts,)),
            dma((2,)),
            dma((2,)),
            dma((3,)),
            dma((3,)),
            dma((3, plan.bits)),
            dma((3, plan.bits)),
            dma((parts, 2, n)),
            dma((parts, 2, n)),
            dma((parts, plan.groups, n)),
            dma((parts, plan.groups, n)),
        ],
        compiler_params=pltpu.CompilerParams(
            collective_id=0, has_side_effects=True, vmem_limit_bytes=60 * 2**20
        ),
        name="flow",
    )(
        latents,
        spectrum,
        *weights,
        embed,
        ids,
        step_row,
        bands,
        bands.transpose(0, 2, 1),
        widened_values(cas_values(HH), plan.sub),
        widened_values(cas_values(TT), TILE),
    )


def finish_kernel(
    plan,
    done,
    back,
    tables,
    gate,
    rest,
    latents,
    out,
    arrived,
    table,
    scale,
    weight,
    residual,
    result,
    held,
    back_sem,
    table_sem,
    scale_sem,
    weight_sem,
    residual_sem,
    result_sem,
    held_in,
    held_out,
):
    n, channels, parts = plan.n, plan.channels, plan.parts
    rows = plan.group * WW
    first = (plan.groups - 1) * rows
    chunk = min(256, rows)
    copy = pltpu.make_async_copy
    count = rows // chunk
    inward = [
        copy(back.at[p, :, pl.ds((plan.groups - 1) * TILE, TILE), :], arrived.at[p], back_sem.at[p])
        for p in range(parts)
    ]
    weight_in = copy(rest.at[:, 1], weight, weight_sem)
    steps = []
    for i in range(count):
        some = pl.ds(i * chunk, chunk)
        steps.append(
            [
                copy(tables.at[:, some, :], table.at[:, some, :], table_sem.at[i]),
                copy(gate.at[some, :], scale.at[some, :], scale_sem.at[i]),
                copy(
                    latents.at[pl.ds(first + i * chunk, chunk), :],
                    residual.at[some, :],
                    residual_sem.at[i],
                ),
            ]
        )
    passing = range(plan.groups - 1)
    into = [copy(done.at[pl.ds(k * rows, rows), :], held.at[k], held_in.at[k]) for k in passing]
    onward = [copy(held.at[k], out.at[pl.ds(k * rows, rows), :], held_out.at[k]) for k in passing]
    for one in (*inward, steps[0][0], weight_in, *steps[0][1:]):
        one.start()
    for step in steps[1:]:
        for one in step:
            one.start()
    for one in into:
        one.start()
    for one in inward:
        one.wait()
    results = []
    for i in range(count):
        some = pl.ds(i * chunk, chunk)
        for one in steps[i]:
            one.wait()
        mix = 0.0
        for p in range(parts):
            mix += dot(table[p, some, :], arrived[p].reshape(n * TILE, channels))
        mixed = (mix * scale[some, :].astype(jnp.float32)).astype(jnp.bfloat16)
        if i == 0:
            weight_in.wait()
        projected = dot(mixed, weight[...].reshape(channels, channels))
        total = residual[some, :].astype(jnp.float32) + projected
        result[some, :] = total.astype(jnp.bfloat16)
        results.append(
            copy(
                result.at[some, :], out.at[pl.ds(first + i * chunk, chunk), :], result_sem.at[i]
            )
        )
        results[-1].start()
        for k in passing:
            if k % count == i:
                into[k].wait()
                onward[k].start()
    for one in (*results, *onward):
        one.wait()


def finish(plan, done, back, tables, gate, rest, latents):
    n, channels, parts = plan.n, plan.channels, plan.parts
    rows = plan.group * WW
    count = rows // min(256, rows)
    bf, vmem, dma = jnp.bfloat16, pltpu.VMEM, pltpu.SemaphoreType.DMA
    return pl.pallas_call(
        lambda *refs: finish_kernel(plan, *refs),
        in_specs=[pl.BlockSpec(memory_space=ANY)] * 6,
        out_specs=pl.BlockSpec(memory_space=ANY),
        out_shape=jax.ShapeDtypeStruct(latents.shape, bf),
        scratch_shapes=[
            vmem((parts, n, TILE, channels), bf),
            vmem(tables.shape, bf),
            vmem((rows, channels), bf),
            vmem((n, plan.depth, channels), bf),
            vmem((rows, channels), bf),
            vmem((rows, channels), bf),
            vmem((plan.groups - 1, rows, channels), bf),
            dma((parts,)),
            dma((count,)),
            dma((count,)),
            dma,
            dma((count,)),
            dma((count,)),
            dma((plan.groups - 1,)),
            dma((plan.groups - 1,)),
        ],
        compiler_params=pltpu.CompilerParams(vmem_limit_bytes=60 * 2**20),
        name="finish",
    )(done, back, tables, gate, rest, latents)


def streamed(latents, spectrum, w_value, w_gate, w_out, embed_table, prompt_ids, noise_step):
    rows, channels = latents.shape
    plan = Plan(lax.axis_size("sp"), rows, channels)
    channel = jnp.arange(channels, dtype=jnp.int32)
    step_row = step_embedding(noise_step, channel, C)[None, :]
    outs = flow(
        plan,
        latents,
        spectrum,
        (w_value, w_gate, w_out),
        embed_table,
        prompt_ids[None, :],
        step_row,
    )
    _, _, _, back, done, _, rest, _, tables, gate = outs
    return finish(plan, done, back, tables, gate, rest, latents)


def fits(mesh):
    n = mesh.shape["sp"]
    alone = mesh.shape["grp"] == 1 and mesh.shape["ch"] == 1
    band = WW // n
    return alone and n >= 8 and n & (n - 1) == 0 and band >= 2 and TT * HH // n * band >= 4 * TILE


def exchange(blocks):
    return lax.all_to_all(blocks, "sp", split_axis=0, concat_axis=0, tiled=True)


def local(latents, spectrum, w_value, w_gate, w_out, embed_table, prompt_ids, noise_step):
    row_count, channels = latents.shape
    chan_part = w_value.shape[1]
    owners = lax.axis_size("sp")
    splits = lax.axis_size("ch")
    lines = row_count // WW
    band = WW // owners
    group = min(lines, max(1, TILE // band))

    parts = 2 if band % 2 == 0 else 1
    sub = band // parts

    table = cas_table(WW).reshape(owners, parts, 1, sub, 1, WW)
    same_line = jnp.eye(group, dtype=jnp.bfloat16).reshape(1, group, 1, group, 1)
    width_tables = [
        (table[:, part] * same_line).reshape(owners * group * sub, group * WW)
        for part in range(parts)
    ]
    height_table = widened(cas_table(HH), sub)
    time_table = widened(cas_table(TT), TILE)
    gains = spectrum.reshape(TT, HH, parts, sub, chan_part)

    full_value = lax.all_gather(w_value, "sp", axis=0)

    full_gate = lax.all_gather(w_gate, "sp", axis=0)
    local_pool = jnp.mean(jnp.take(embed_table, prompt_ids, axis=1).astype(jnp.float32), axis=1)
    offset = lax.axis_index("ch") * chan_part
    depth = w_out.shape[0]
    if splits == 1:
        first = local_pool.astype(jnp.bfloat16)
        rest = local_pool - first.astype(jnp.float32)
        second = rest.astype(jnp.bfloat16)
        third = (rest - second.astype(jnp.float32)).astype(jnp.bfloat16)
        terms = jnp.stack([first, second, third])
        terms = jnp.pad(terms, ((0, TILE - 3), (0, channels - terms.shape[1])))
        full_out = lax.all_gather(jnp.concatenate([w_out, terms], axis=0), "sp", axis=0)
    else:
        pooled_all = lax.all_gather(local_pool, ("sp", "ch"), axis=0, tiled=True)
        pooled = lax.dynamic_slice_in_dim(pooled_all, offset, chan_part)
        rows_out = lax.all_gather(w_out, "sp", axis=0, tiled=True)
        full_out = lax.dynamic_slice_in_dim(rows_out, offset, chan_part, 0)[None]
        depth = chan_part

    planes, backs = [], []
    for part in range(parts):
        sent = width_forward(width_tables[part], latents, owners, lines, sub, group)
        if planes:
            sent, planes[-1], full_value = lax.optimization_barrier((sent, planes[-1], full_value))
        planes.append(exchange(sent))
    for part in range(parts):
        filtered = plane_filter(
            height_table,
            time_table,
            planes[part].reshape(TT * HH * sub, channels),
            full_value,
            gains[:, :, part].reshape(TT, HH * sub, chan_part),
            sub,
        ).reshape(owners, lines * sub, chan_part)
        if backs:
            filtered, backs[-1], full_gate = lax.optimization_barrier(
                (filtered, backs[-1], full_gate)
            )
        elif parts > 1:
            filtered, planes[-1], full_out = lax.optimization_barrier(
                (filtered, planes[-1], full_out)
            )
        backs.append(exchange(filtered))

    if splits == 1:
        pooled = full_out[:, depth : depth + 3, : local_pool.shape[0]].astype(jnp.float32)
        pooled = jnp.sum(pooled, axis=1).reshape(chan_part)
    channel = offset + jnp.arange(chan_part, dtype=jnp.int32)
    modulation = 1.0 + pooled + step_embedding(noise_step, channel, C)

    gate = gate_rows(latents, full_gate, modulation[None, :])
    mixed = mix_and_project(
        [width_table.T for width_table in width_tables],
        backs,
        latents,
        gate,
        full_out,
        depth,
        group,
        splits == 1,
    )
    if splits == 1:
        return mixed
    half_rows = row_count // splits
    summed = lax.psum_scatter(mixed, "ch", scatter_dimension=0, tiled=True).astype(jnp.float32)
    residual = lax.dynamic_slice_in_dim(latents, lax.axis_index("ch") * half_rows, half_rows, 0)
    return (residual.astype(jnp.float32) + summed).astype(jnp.bfloat16)


def solution(mesh):
    placed = (
        P(("grp", "sp"), None),
        P(None, None, "sp", "ch"),
        P("sp", "ch"),
        P("sp", "ch"),
        P("sp", None),
        P(("sp", "ch"), None),
        P("grp"),
        P("grp"),
    )
    return jax.shard_map(
        streamed if fits(mesh) else local,
        mesh=mesh, in_specs=placed, out_specs=P(("grp", "sp", "ch"), None), check_vma=False
    )
```
